32 devices in a mesh: gx: 4 (over y, x), gy: 4 (over z), gz: 2 (over core).
Axes of the slice: x: 2, y: 2, z: 4, core: 2. Of those that a mesh axis runs over, the one named last changes fastest.
Arguments:
- ref_image: bfloat16 [1024, 64, 256], P('gx', 'gy', 'gz'), may hold values from -6 to 6
- def_image: bfloat16 [1024, 64, 256], P('gx', 'gy', 'gz'), may hold values from -6 to 6
- displacement: float32 [3, 128, 8, 32], P(None, 'gx', 'gy', 'gz'), may hold values from -3 to 3
Outputs:
- new_displacement: float32 [3, 128, 8, 32], P(None, 'gx', 'gy', 'gz')
- fine_residual: bfloat16 [1024, 64, 256], P('gx', 'gy', 'gz')
The draws below stay inside these ranges and needn't reach their ends.
All inputs are finite; a program needn't handle non-finite values.
Results may differ from the reference program's by a relative error of at most 0.0022.
Values may be sent and summed in bfloat16 or wider, within the bound.
A program may use at most 64 MiB of HBM per device.

```python
import jax
import jax.numpy as jnp
from jax import lax

NX = 1024
NY = 64
NZ = 256
MX = 128
MY = 8
MZ = 32


def steps_of(stream_key, dims, pieces, low, high):
    def one(position, parts):
        draws = jax.random.uniform(jax.random.fold_in(jax.random.fold_in(stream_key, 6), position), (parts,), jnp.float32, low / len(pieces), high / len(pieces))
        return jnp.repeat(jnp.exp(draws), dims[position] // parts).reshape((-1,) + (1,) * (len(dims) - position - 1))

    factor_of = one(*pieces[0])
    for cut in pieces[1:]:
        factor_of = factor_of * one(*cut)
    return factor_of


def noise(rng, extent, width, most, pieces=(), kind=jnp.bfloat16):
    values = jax.random.normal(rng, extent, jnp.float32) * width
    if len(pieces) > 0:
        values = steps_of(rng, extent, pieces, -0.22, 0.18) * values
    return jnp.clip(values, min=-most, max=most).astype(kind)


def setup_inputs(seed: int = 0) -> dict:
    key_list = jax.random.split(jax.random.key(seed), 4)
    return {
        "ref_image": noise(key_list[0], (NX, NY, NZ), 1.0, 6.0, ((0, 4), (1, 4), (2, 2))),
        "def_image": noise(key_list[1], (NX, NY, NZ), 1.0, 6.0, ((0, 4), (1, 4), (2, 2))),
        "displacement": noise(key_list[2], (3, MX, MY, MZ), 0.5, 3.0, ((1, 4), (2, 4), (3, 2)), jnp.float32),
    }


stiffness = 64.0

def bin_level(image):
    values = image.astype(jnp.float32)
    sizex, sizey, sizez = values.shape
    return values.reshape(sizex // 8, 8, sizey // 8, 8, sizez // 8, 8).sum((1, 3, 5)) / 32.0

def central(padded):
    slope_x = (padded[2:, 1:-1, 1:-1] - padded[:-2, 1:-1, 1:-1]) / 2.0
    slope_y = (padded[1:-1, 2:, 1:-1] - padded[1:-1, :-2, 1:-1]) / 2.0
    slope_z = (padded[1:-1, 1:-1, 2:] - padded[1:-1, 1:-1, :-2]) / 2.0
    return (slope_x, slope_y, slope_z)

def line_matrix(count):
    return jnp.eye(count, dtype=jnp.float32) * (1.0 + 2.0 * stiffness) - stiffness * (jnp.eye(count, k=1, dtype=jnp.float32) + jnp.eye(count, k=-1, dtype=jnp.float32))

def prolong_table(fine_count, coarse_count):
    index = jnp.arange(fine_count)
    center = index // 8 + 1
    offset = ((index % 8).astype(jnp.float32) + 0.5) / 8.0 - 0.5
    column = jnp.arange(coarse_count + 2)[None, :]
    weight = jnp.where(column == center[:, None], 1.0 - jnp.abs(offset)[:, None], 0.0)
    weight = weight + jnp.where((offset[:, None] >= 0.0) & (column == center[:, None] + 1), offset[:, None], 0.0)
    weight = weight + jnp.where((offset[:, None] < 0.0) & (column == center[:, None] - 1), -offset[:, None], 0.0)
    return weight.astype(jnp.float32)

def reference(ref_image, def_image, displacement):
    coarse_ref = bin_level(ref_image)
    coarse_def = bin_level(def_image)
    slopes = central(jnp.pad(coarse_ref, 1))
    mismatch = coarse_def - coarse_ref - (slopes[0] * displacement[0] + slopes[1] * displacement[1] + slopes[2] * displacement[2])
    rhs = jnp.stack([slope * mismatch for slope in slopes])
    lines = rhs.shape[1]
    factor = jnp.linalg.cholesky(line_matrix(lines))
    flat = jnp.moveaxis(rhs, 1, 0).reshape(lines, -1)
    solved = jax.scipy.linalg.cho_solve((factor, True), flat)
    step = jnp.moveaxis(solved.reshape(lines, 3, rhs.shape[2], rhs.shape[3]), 0, 1)
    new_displacement = displacement + step
    padded = jnp.pad(new_displacement, ((0, 0), (1, 1), (1, 1), (1, 1)))
    table_x = prolong_table(ref_image.shape[0], rhs.shape[1])
    table_y = prolong_table(ref_image.shape[1], rhs.shape[2])
    table_z = prolong_table(ref_image.shape[2], rhs.shape[3])
    grads = central(jnp.pad(ref_image.astype(jnp.float32), 1))
    total = def_image.astype(jnp.float32) - ref_image.astype(jnp.float32)
    for component in range(3):
        field = jnp.einsum('ia,abc->ibc', table_x, padded[component], precision=lax.Precision.HIGHEST)
        field = jnp.einsum('jb,ibc->ijc', table_y, field, precision=lax.Precision.HIGHEST)
        field = jnp.einsum('ijc,kc->ijk', field, table_z, precision=lax.Precision.HIGHEST)
        total = total - grads[component] * field
    return (new_displacement, total.astype(jnp.bfloat16))
```

```python
import functools

import jax
import jax.numpy as jnp
import numpy as np
from jax import lax
from jax.experimental import pallas as pl
from jax.experimental.pallas import tpu as pltpu
from jax.sharding import PartitionSpec as P

stiffness = 64.0
BIN = 8
SLOT = 32
MESH = pl.DeviceIdType.MESH
HIGHEST = lax.Precision.HIGHEST


def inverse_table(devices, cells):
    lines = devices * cells
    theta = np.arccosh((1.0 + 2.0 * stiffness) / (2.0 * stiffness))
    index = np.arange(lines)
    low = np.minimum(index[:, None], index[None, :])
    high = np.maximum(index[:, None], index[None, :])
    a, b, c = (low + 1) * theta, (lines - high) * theta, (lines + 1) * theta
    inverse = (
        np.exp(a + b - c) * (1 - np.exp(-2 * a)) * (1 - np.exp(-2 * b)) / (1 - np.exp(-2 * c))
        / (2.0 * stiffness * np.sinh(theta))
    )
    table = np.zeros((devices, 3, cells + 16, cells + 8 * devices))
    sums = np.zeros((devices, 8, 3 * cells))
    for me in range(devices):
        first, last = me * cells, (me + 1) * cells - 1
        own = index[first : last + 1]
        up = np.exp((own - last) * theta) * (1 - np.exp(-2 * (own + 1) * theta)) / (1 - np.exp(-2 * (last + 1) * theta))
        down = (
            np.exp((first - own) * theta)
            * (1 - np.exp(-2 * (lines - own) * theta))
            / (1 - np.exp(-2 * (lines - first) * theta))
        )
        for k in range(3):
            sums[me, 2 * k, k * cells : (k + 1) * cells] = up
            sums[me, 2 * k + 1, k * cells : (k + 1) * cells] = down
            for row in range(7, cells + 9):
                x = first + row - 8
                if x < 0 or x >= lines:
                    continue
                table[me, k, row, :cells] = inverse[x, first : last + 1]
                for peer in range(devices):
                    if peer < me:
                        table[me, k, row, cells + 8 * peer + 2 * k] = inverse[x, (peer + 1) * cells - 1]
                    if peer > me:
                        table[me, k, row, cells + 8 * peer + 2 * k + 1] = inverse[x, peer * cells]
    return table.astype(np.float32), sums.astype(np.float32)


def lane_tables(cells_z, size_z, slots):
    place = np.zeros((cells_z, 3 * 128), np.float32)
    for variant in range(3):
        for z in range(cells_z):
            lane = z + 2 - (variant - 1) * cells_z
            if 0 <= lane < cells_z + 4:
                place[z, variant * 128 + lane] = 1.0
    binning = np.repeat(place, BIN, axis=0) / 32.0
    prolong = np.zeros((128, slots * size_z), np.float32)
    for slot in range(slots):
        for fine in range(size_z):
            lane, offset = slot * SLOT + fine // BIN + 2, (fine % BIN + 0.5) / BIN - 0.5
            prolong[lane, slot * size_z + fine] = 1.0 - abs(offset)
            prolong[lane + (1 if offset >= 0 else -1), slot * size_z + fine] = abs(offset)
    return place, binning, prolong


def kernel(
    counts,
    ref_ref, def_ref, disp_ref, table_ref, sums_ref, place_ref, bin_ref, prolong_ref,
    new_ref, out_ref,
    volume, binned, packed, halo, mine, theirs, xhalo, ysend, yhalo, zhalo, lines,
    near_send, near_recv, peer_send, peer_recv, x_send, x_recv, y_send, y_recv, z_send, z_recv,
):
    nx, ny, nz = counts
    sizex, sizey, sizez = ref_ref.shape
    cells_x, cells_z = sizex // BIN, sizez // BIN
    pitch = sizey + 16
    me = (lax.axis_index("gx"), lax.axis_index("gy"), lax.axis_index("gz"))

    def inside(offset):
        good = None
        for at, step, count in zip(me, offset, counts):
            if step:
                test = at > 0 if step < 0 else at < count - 1
                good = test if good is None else jnp.logical_and(good, test)
        return good

    def device(offset):
        return {"gx": me[0] + offset[0], "gy": me[1] + offset[1], "gz": me[2] + offset[2]}

    def peer(j):
        return {"gx": lax.rem(me[0] + j, nx), "gy": me[1], "gz": me[2]}

    steps = (-1, 0, 1)
    offsets = [(i, j, k) for i in steps for j in steps for k in steps if (i, j, k) != (0, 0, 0)]

    halo[...] = jnp.zeros_like(halo)
    theirs[...] = jnp.zeros_like(theirs)
    xhalo[...] = jnp.zeros_like(xhalo)
    yhalo[...] = jnp.zeros_like(yhalo)

    z_steps = (1,) if nz == 2 else (1, nz - 1)

    def z_device(step):
        return {"gx": me[0], "gy": me[1], "gz": lax.rem(me[2] + step, nz)}

    barrier = pltpu.get_barrier_semaphore()
    for j in range(1, nx):
        pl.semaphore_signal(barrier, inc=1, device_id=peer(j), device_id_type=MESH)
    expect = jnp.int32(nx - 1)
    for offset in offsets:
        if offset[1:] == (0, 0):
            continue

        @pl.when(inside(offset))
        def _():
            pl.semaphore_signal(barrier, inc=1, device_id=device(offset), device_id_type=MESH)

    reach = [
        1 + (at > 0).astype(jnp.int32) + (at < count - 1).astype(jnp.int32)
        for at, count in zip(me, counts)
    ]
    expect = expect + reach[0] * (reach[1] * reach[2] - 1)
    if nz > 2:
        ends = jnp.logical_or(me[2] == 0, me[2] == nz - 1)

        @pl.when(ends)
        def _():
            other = {"gx": me[0], "gy": me[1], "gz": nz - 1 - me[2]}
            pl.semaphore_signal(barrier, inc=1, device_id=other, device_id_type=MESH)

        expect = expect + ends.astype(jnp.int32)
    pl.semaphore_wait(barrier, expect)

    z_copies = [
        pltpu.make_async_remote_copy(
            src_ref=ref_ref, dst_ref=zhalo.at[i], send_sem=z_send.at[i], recv_sem=z_recv.at[i],
            device_id=z_device(step), device_id_type=MESH,
        )
        for i, step in enumerate(z_steps)
    ]

    source_rows = {-1: (0, 8), 0: (0, cells_x), 1: (cells_x - 8, 8)}
    target_rows = {-1: (0, 8), 0: (8, cells_x), 1: (cells_x + 8, 8)}

    def number(offset):
        return (offset[0] + 1) * 9 + (offset[1] + 1) * 3 + offset[2] + 1

    def near_copy(offset, part):
        blocks = pl.ds(0, 1) if part == 0 else pl.ds(1, 2)
        back = tuple(-step for step in offset)
        start, rows = source_rows[offset[0]]
        goal = target_rows[back[0]][0]
        return pltpu.make_async_remote_copy(
            src_ref=packed.at[offset[2] + 1, blocks, pl.ds(start, rows), :],
            dst_ref=halo.at[back[1] + 1, back[2] + 1, blocks, pl.ds(goal, rows), :],
            send_sem=near_send.at[number(offset), part],
            recv_sem=near_recv.at[number(back), part],
            device_id=device(offset), device_id_type=MESH,
        )

    def near_arrival(offset, part):
        blocks = pl.ds(0, 1) if part == 0 else pl.ds(1, 2)
        goal, rows = target_rows[offset[0]]
        where = halo.at[offset[1] + 1, offset[2] + 1, blocks, pl.ds(goal, rows), :]
        return pltpu.make_async_remote_copy(
            src_ref=where, dst_ref=where,
            send_sem=near_send.at[number(offset), part],
            recv_sem=near_recv.at[number(offset), part],
            device_id=device(offset), device_id_type=MESH,
        )

    def pack(lines_of):
        total = None
        for q, line in enumerate(lines_of):
            spread = jnp.dot(line, place_ref[...], precision=HIGHEST, preferred_element_type=jnp.float32)
            spread = [spread[:, 128 * v : 128 * (v + 1)] for v in range(3)]
            if q:
                spread = [pltpu.roll(s, SLOT * q, 1) for s in spread]
            total = spread if total is None else [t + s for t, s in zip(total, spread)]
        return total

    pairs = [(k, y) for k in range(3) for y in range(2)]
    for block, members in ((1, pairs[:4]), (2, pairs[4:])):
        spread = pack([disp_ref[k, :, y, :] for k, y in members])
        for v in range(3):
            packed[v, block] = spread[v]
        halo[1, 1, block, pl.ds(8, cells_x), :] = spread[1]
    for offset in offsets:

        @pl.when(inside(offset))
        def _():
            near_copy(offset, 1).start()

    def x_copy(step):
        return pltpu.make_async_remote_copy(
            src_ref=ref_ref.at[pl.ds(sizex - 1 if step > 0 else 0, 1)],
            dst_ref=xhalo.at[pl.ds(0 if step > 0 else 1, 1)],
            send_sem=x_send.at[0 if step > 0 else 1], recv_sem=x_recv.at[0 if step > 0 else 1],
            device_id=device((step, 0, 0)), device_id_type=MESH,
        )

    for step in (-1, 1):

        @pl.when(inside((step, 0, 0)))
        def _():
            x_copy(step).start()

    for copy in z_copies:
        copy.start()

    def bin_cell(cell, carry):
        rows = pl.multiple_of(cell * 8, 8)
        total = [None, None]
        for i in range(BIN):
            x = cell * BIN + i
            slabs = (ref_ref[x].astype(jnp.float32), def_ref[x].astype(jnp.float32))
            volume[pl.ds(pl.multiple_of((x + 1) * pitch + 8, 8), sizey), :] = slabs[0]
            total = [s if t is None else t + s for t, s in zip(total, slabs)]
        for image in range(2):
            for y in range(2):
                binned[2 * image + y, pl.ds(rows, 8), :] = total[image][8 * y : 8 * y + 8]
        return carry

    lax.fori_loop(0, cells_x, bin_cell, 0)
    spread = None
    for q in range(4):
        line = binned[q, pl.ds(0, cells_x, stride=8), :]
        for s in range(1, 8):
            line = line + binned[q, pl.ds(s, cells_x, stride=8), :]
        part = jnp.dot(line, bin_ref[...], precision=HIGHEST, preferred_element_type=jnp.float32)
        part = [part[:, 128 * v : 128 * (v + 1)] for v in range(3)]
        if q:
            part = [pltpu.roll(p, SLOT * q, 1) for p in part]
        spread = part if spread is None else [a + b for a, b in zip(spread, part)]
    for v in range(3):
        packed[v, 0] = spread[v]
    halo[1, 1, 0, pl.ds(8, cells_x), :] = spread[1]
    for offset in offsets:

        @pl.when(inside(offset))
        def _():
            near_copy(offset, 0).start()

    def y_copy(step):
        side = 1 if step > 0 else 0
        return pltpu.make_async_remote_copy(
            src_ref=ysend.at[side], dst_ref=yhalo.at[1 - side],
            send_sem=y_send.at[side], recv_sem=y_recv.at[1 - side],
            device_id=device((0, step, 0)), device_id_type=MESH,
        )

    ysend[0] = volume[pl.ds(pitch + 8, sizex, stride=pitch), :].astype(jnp.bfloat16)
    ysend[1] = volume[pl.ds(pitch + 7 + sizey, sizex, stride=pitch), :].astype(jnp.bfloat16)
    for step in (-1, 1):

        @pl.when(inside((0, step, 0)))
        def _():
            y_copy(step).start()

    for part in (1, 0):
        for offset in offsets:

            @pl.when(inside(offset))
            def _():
                near_arrival(offset, part).wait_recv()

    summed = [[halo[y, 0, b] + halo[y, 1, b] + halo[y, 2, b] for b in range(3)] for y in range(3)]
    rows = cells_x + 16
    lane = lax.broadcasted_iota(jnp.int32, (rows, 128), 1)
    slot = lane // SLOT

    def centred(b, upper):
        one, two = (SLOT, 128 - SLOT) if upper else (128 - SLOT, SLOT)
        ends = jnp.where(slot == 0, pltpu.roll(summed[0][b], one, 1), pltpu.roll(summed[2][b], one, 1))
        return jnp.where(jnp.logical_or(slot == 0, slot == 3), ends, pltpu.roll(summed[1][b], two, 1))

    coarse = centred(0, False)
    deformed = centred(0, True)
    displacement = [centred(1, False), centred(1, True), centred(2, False)]
    before = jnp.where(slot < 2, summed[0][0], pltpu.roll(summed[1][0], 64, 1))
    after = jnp.where(slot < 2, summed[1][0], pltpu.roll(summed[2][0], 64, 1))
    slopes = [
        (pltpu.roll(coarse, rows - 1, 0) - pltpu.roll(coarse, 1, 0)) * 0.5,
        (after - before) * 0.5,
        (pltpu.roll(coarse, 127, 1) - pltpu.roll(coarse, 1, 1)) * 0.5,
    ]
    mismatch = deformed - coarse - (
        slopes[0] * displacement[0] + slopes[1] * displacement[1] + slopes[2] * displacement[2]
    )
    place = lane - slot * SLOT
    low = jnp.where(me[2] > 0, 1, 2)
    high = jnp.where(me[2] < nz - 1, cells_z + 2, cells_z + 1)
    keep = jnp.logical_and(place >= low, place <= high)
    keep = jnp.logical_and(keep, slot >= jnp.where(me[1] > 0, 0, 1))
    keep = jnp.logical_and(keep, slot <= jnp.where(me[1] < ny - 1, 3, 2))
    rhs = [jnp.where(keep, s * mismatch, 0.0)[8 : 8 + cells_x] for s in slopes]

    mine[...] = jnp.dot(
        sums_ref[me[0]], jnp.concatenate(rhs, axis=0), precision=HIGHEST, preferred_element_type=jnp.float32
    )

    def peer_copy(j):
        return pltpu.make_async_remote_copy(
            src_ref=mine, dst_ref=theirs.at[me[0]],
            send_sem=peer_send.at[j], recv_sem=peer_recv.at[j],
            device_id=peer(j), device_id_type=MESH,
        )

    for j in range(1, nx):
        peer_copy(j).start()

    for step in (-1, 1):

        @pl.when(inside((step, 0, 0)))
        def _():
            x_copy(-step).wait_recv()

        @pl.when(inside((0, step, 0)))
        def _():
            y_copy(-step).wait_recv()

    volume[pl.ds(8, sizey), :] = xhalo[0].astype(jnp.float32)
    volume[pl.ds((sizex + 1) * pitch + 8, sizey), :] = xhalo[1].astype(jnp.float32)
    volume[pl.ds(pitch + 7, sizex, stride=pitch), :] = yhalo[0].astype(jnp.float32)
    volume[pl.ds(pitch + 8 + sizey, sizex, stride=pitch), :] = yhalo[1].astype(jnp.float32)

    row = lax.broadcasted_iota(jnp.int32, (sizez, sizez), 0)
    column = lax.broadcasted_iota(jnp.int32, (sizez, sizez), 1)
    inner = jnp.where(row == column + 1, 1.0, 0.0) - jnp.where(row + 1 == column, 1.0, 0.0)
    from_low = jnp.where(
        jnp.logical_and(jnp.logical_and(row == sizez - 1, column == 0), me[2] > 0), -1.0, 0.0
    )
    from_high = jnp.where(
        jnp.logical_and(jnp.logical_and(row == 0, column == sizez - 1), me[2] < nz - 1), 1.0, 0.0
    )
    outer = [from_low + from_high] if nz == 2 else [from_low, from_high]
    across = jnp.concatenate([inner] + outer, axis=0).astype(jnp.bfloat16)

    for j in range(1, nx):
        came = pltpu.make_async_remote_copy(
            src_ref=mine, dst_ref=theirs.at[lax.rem(me[0] + nx - j, nx)],
            send_sem=peer_send.at[j], recv_sem=peer_recv.at[j],
            device_id=peer(j), device_id_type=MESH,
        )
        came.wait_recv()

    sums = theirs[...].reshape(8 * nx, 128)
    for k in range(3):
        step = jnp.dot(
            table_ref[me[0], k], jnp.concatenate([rhs[k], sums], axis=0),
            precision=HIGHEST, preferred_element_type=jnp.float32,
        )
        new = displacement[k] + step
        for y in range(2):
            shift = 128 - SLOT * (y + 1) - 2
            new_ref[k, :, y, :] = pltpu.roll(new, shift, 1)[8 : 8 + cells_x, :cells_z]
        along = jnp.dot(new, prolong_ref[...], precision=HIGHEST, preferred_element_type=jnp.float32) * 0.5
        for s in range(4):
            lines[k, s] = along[:, sizez * s : sizez * (s + 1)]

    for copy in z_copies:
        copy.wait_recv()

    third = lax.broadcasted_iota(jnp.int32, (8, sizez), 0).astype(jnp.float32)
    offset_y = (third + 0.5) / 8.0 - 0.5
    weight_low = jnp.maximum(-offset_y, 0.0)
    weight_high = jnp.maximum(offset_y, 0.0)
    weight_mid = 1.0 - jnp.abs(offset_y)

    def plane(at):
        planes = []
        for k in range(3):
            row_of = [lines[k, s, pl.ds(at, 1), :] for s in range(4)]
            planes.append(
                jnp.concatenate(
                    [
                        weight_low * row_of[c] + weight_mid * row_of[c + 1] + weight_high * row_of[c + 2]
                        for c in range(2)
                    ],
                    axis=0,
                )
            )
        return planes

    def residual(cell, carry):
        past, now = carry
        later = plane(cell + 9)
        slabs = pl.ds(cell * BIN, BIN)
        images = [ref_ref[slabs].reshape(BIN * sizey, sizez)] + [
            zhalo[i, slabs].reshape(BIN * sizey, sizez) for i in range(len(z_steps))
        ]
        grad_z = jnp.dot(jnp.concatenate(images, axis=1), across, preferred_element_type=jnp.float32)
        for i in range(BIN):
            t = (i + 0.5) / BIN - 0.5
            other = later if t > 0 else past
            field = [n + abs(t) * (o - n) for n, o in zip(now, other)]
            x = cell * BIN + i
            base = pl.multiple_of((x + 1) * pitch, 8)
            centre = volume[pl.ds(base + 8, sizey), :]
            grad_x = volume[pl.ds(base + pitch + 8, sizey), :] - volume[pl.ds(base - pitch + 8, sizey), :]
            grad_y = volume[pl.ds(base + 9, sizey), :] - volume[pl.ds(base + 7, sizey), :]
            total = def_ref[x].astype(jnp.float32) - centre
            total = total - grad_x * field[0] - grad_y * field[1]
            total = total - grad_z[i * sizey : (i + 1) * sizey] * field[2]
            out_ref[x] = total.astype(jnp.bfloat16)
        return (now, later)

    lax.fori_loop(0, cells_x, residual, (plane(7), plane(8)))

    for copy in z_copies:
        copy.wait_send()
    for j in range(1, nx):
        peer_copy(j).wait_send()
    for step in (-1, 1):

        @pl.when(inside((step, 0, 0)))
        def _():
            x_copy(step).wait_send()

        @pl.when(inside((0, step, 0)))
        def _():
            y_copy(step).wait_send()

    for offset in offsets:

        @pl.when(inside(offset))
        def _():
            for part in range(2):
                near_copy(offset, part).wait_send()


def on_device(counts, ref_image, def_image, displacement):
    nx, ny, nz = counts
    sizex, sizey, sizez = ref_image.shape
    cells_x, cells_z = sizex // BIN, sizez // BIN
    table, sums = inverse_table(nx, cells_x)
    place, binning, prolong = lane_tables(cells_z, sizez, 4)
    sides = 1 if nz == 2 else 2
    dma = pltpu.SemaphoreType.DMA
    vmem = pl.BlockSpec(memory_space=pltpu.VMEM)
    return pl.pallas_call(
        functools.partial(kernel, counts),
        out_shape=(
            jax.ShapeDtypeStruct(displacement.shape, jnp.float32),
            jax.ShapeDtypeStruct(ref_image.shape, jnp.bfloat16),
        ),
        in_specs=[vmem] * 8,
        out_specs=(vmem, vmem),
        scratch_shapes=[
            pltpu.VMEM(((sizex + 2) * (sizey + 16), sizez), jnp.float32),
            pltpu.VMEM((4, cells_x * 8, sizez), jnp.float32),
            pltpu.VMEM((3, 3, cells_x, 128), jnp.float32),
            pltpu.VMEM((3, 3, 3, cells_x + 16, 128), jnp.float32),
            pltpu.VMEM((8, 128), jnp.float32),
            pltpu.VMEM((nx, 8, 128), jnp.float32),
            pltpu.VMEM((2, sizey, sizez), jnp.bfloat16),
            pltpu.VMEM((2, sizex, sizez), jnp.bfloat16),
            pltpu.VMEM((2, sizex, sizez), jnp.bfloat16),
            pltpu.VMEM((sides, sizex, sizey, sizez), jnp.bfloat16),
            pltpu.VMEM((3, 4, cells_x + 16, sizez), jnp.float32),
            dma((27, 2)), dma((27, 2)), dma((nx,)), dma((nx,)),
            dma((2,)), dma((2,)), dma((2,)), dma((2,)), dma((sides,)), dma((sides,)),
        ],
        compiler_params=pltpu.CompilerParams(collective_id=0, has_side_effects=True),
    )(ref_image, def_image, displacement, table, sums, place, binning, prolong)


def solution(mesh):
    counts = tuple(mesh.shape[axis] for axis in ("gx", "gy", "gz"))
    return jax.shard_map(
        functools.partial(on_device, counts),
        mesh=mesh,
        in_specs=(P("gx", "gy", "gz"), P("gx", "gy", "gz"), P(None, "gx", "gy", "gz")),
        out_specs=(P(None, "gx", "gy", "gz"), P("gx", "gy", "gz")),
        check_vma=False,
    )
```

```python
import functools

import jax
import jax.numpy as jnp
import numpy as np
from jax import lax
from jax.experimental import pallas as pl
from jax.experimental.pallas import tpu as pltpu
from jax.sharding import PartitionSpec as P

stiffness = 64.0
BIN = 8
SLOT = 32
MESH = pl.DeviceIdType.MESH
HIGHEST = lax.Precision.HIGHEST


def inverse_table(devices, cells):
    lines = devices * cells
    theta = np.arccosh((1.0 + 2.0 * stiffness) / (2.0 * stiffness))
    index = np.arange(lines)
    low = np.minimum(index[:, None], index[None, :])
    high = np.maximum(index[:, None], index[None, :])
    a, b, c = (low + 1) * theta, (lines - high) * theta, (lines + 1) * theta
    inverse = (
        np.exp(a + b - c) * (1 - np.exp(-2 * a)) * (1 - np.exp(-2 * b)) / (1 - np.exp(-2 * c))
        / (2.0 * stiffness * np.sinh(theta))
    )
    table = np.zeros((devices, 3, cells + 16, cells + 8 * devices))
    sums = np.zeros((devices, 8, 3 * cells))
    for me in range(devices):
        first, last = me * cells, (me + 1) * cells - 1
        own = index[first : last + 1]
        up = np.exp((own - last) * theta) * (1 - np.exp(-2 * (own + 1) * theta)) / (1 - np.exp(-2 * (last + 1) * theta))
        down = (
            np.exp((first - own) * theta)
            * (1 - np.exp(-2 * (lines - own) * theta))
            / (1 - np.exp(-2 * (lines - first) * theta))
        )
        for k in range(3):
            sums[me, 2 * k, k * cells : (k + 1) * cells] = up
            sums[me, 2 * k + 1, k * cells : (k + 1) * cells] = down
            for row in range(7, cells + 9):
                x = first + row - 8
                if x < 0 or x >= lines:
                    continue
                table[me, k, row, :cells] = inverse[x, first : last + 1]
                for peer in range(devices):
                    if peer < me:
                        table[me, k, row, cells + 8 * peer + 2 * k] = inverse[x, (peer + 1) * cells - 1]
                    if peer > me:
                        table[me, k, row, cells + 8 * peer + 2 * k + 1] = inverse[x, peer * cells]
    return table.astype(np.float32), sums.astype(np.float32)


def lane_tables(cells_z, size_z, slots):
    place = np.zeros((cells_z, 3 * 128), np.float32)
    for variant in range(3):
        for z in range(cells_z):
            lane = z + 2 - (variant - 1) * cells_z
            if 0 <= lane < cells_z + 4:
                place[z, variant * 128 + lane] = 1.0
    binning = np.repeat(place, BIN, axis=0) / 32.0
    prolong = np.zeros((128, slots * size_z), np.float32)
    for slot in range(slots):
        for fine in range(size_z):
            lane, offset = slot * SLOT + fine // BIN + 2, (fine % BIN + 0.5) / BIN - 0.5
            prolong[lane, slot * size_z + fine] = 1.0 - abs(offset)
            prolong[lane + (1 if offset >= 0 else -1), slot * size_z + fine] = abs(offset)
    return place, binning, prolong


def exchange(
    counts,
    ref_hbm, def_hbm, disp_hbm, table_hbm, sums_hbm, place_hbm, bin_hbm, prolong_hbm,
    new_ref, lines, framed, def_ref, yout, zhalo,
    disp_ref, table_ref, sums_ref, place_ref, bin_ref, prolong_ref,
    binned, packed, halo, mine, theirs, xhalo, yrows, ysend, yhalo,
    load_sem,
    near_send, near_recv, peer_send, peer_recv, x_send, x_recv, y_send, y_recv, z_send, z_recv,
):
    nx, ny, nz = counts
    sizex, sizey, sizez = def_ref.shape
    ref_ref = framed.at[pl.ds(1, sizex)]
    cells_x, cells_z = sizex // BIN, sizez // BIN
    me = (lax.axis_index("gx"), lax.axis_index("gy"), lax.axis_index("gz"))

    def inside(offset):
        good = None
        for at, step, count in zip(me, offset, counts):
            if step:
                test = at > 0 if step < 0 else at < count - 1
                good = test if good is None else jnp.logical_and(good, test)
        return good

    def device(offset):
        return {"gx": me[0] + offset[0], "gy": me[1] + offset[1], "gz": me[2] + offset[2]}

    def peer(j):
        return {"gx": lax.rem(me[0] + j, nx), "gy": me[1], "gz": me[2]}

    steps = (-1, 0, 1)
    offsets = [(i, j, k) for i in steps for j in steps for k in steps if (i, j, k) != (0, 0, 0)]

    loads = [
        pltpu.make_async_copy(hbm, held, load_sem.at[i])
        for i, (hbm, held) in enumerate(
            (
                (disp_hbm, disp_ref), (place_hbm, place_ref), (ref_hbm, ref_ref), (def_hbm, def_ref),
                (bin_hbm, bin_ref), (sums_hbm.at[me[0]], sums_ref),
                (table_hbm.at[me[0]], table_ref), (prolong_hbm, prolong_ref),
            )
        )
    ]
    for load in loads:
        load.start()
    halo[...] = jnp.zeros_like(halo)
    theirs[...] = jnp.zeros_like(theirs)
    xhalo[...] = jnp.zeros_like(xhalo)
    yhalo[...] = jnp.zeros_like(yhalo)

    z_steps = (1,) if nz == 2 else (1, nz - 1)

    def z_device(step):
        return {"gx": me[0], "gy": me[1], "gz": lax.rem(me[2] + step, nz)}

    barrier = pltpu.get_barrier_semaphore()
    for j in range(1, nx):
        pl.semaphore_signal(barrier, inc=1, device_id=peer(j), device_id_type=MESH)
    expect = jnp.int32(nx - 1)
    for offset in offsets:
        if offset[1:] == (0, 0):
            continue

        @pl.when(inside(offset))
        def _():
            pl.semaphore_signal(barrier, inc=1, device_id=device(offset), device_id_type=MESH)

    reach = [
        1 + (at > 0).astype(jnp.int32) + (at < count - 1).astype(jnp.int32)
        for at, count in zip(me, counts)
    ]
    expect = expect + reach[0] * (reach[1] * reach[2] - 1)
    if nz > 2:
        ends = jnp.logical_or(me[2] == 0, me[2] == nz - 1)

        @pl.when(ends)
        def _():
            other = {"gx": me[0], "gy": me[1], "gz": nz - 1 - me[2]}
            pl.semaphore_signal(barrier, inc=1, device_id=other, device_id_type=MESH)

        expect = expect + ends.astype(jnp.int32)
    pl.semaphore_wait(barrier, expect)

    z_copies = [
        pltpu.make_async_remote_copy(
            src_ref=ref_ref, dst_ref=zhalo.at[i], send_sem=z_send.at[i], recv_sem=z_recv.at[i],
            device_id=z_device(step), device_id_type=MESH,
        )
        for i, step in enumerate(z_steps)
    ]

    source_rows = {-1: (0, 8), 0: (0, cells_x), 1: (cells_x - 8, 8)}
    target_rows = {-1: (0, 8), 0: (8, cells_x), 1: (cells_x + 8, 8)}

    def number(offset):
        return (offset[0] + 1) * 9 + (offset[1] + 1) * 3 + offset[2] + 1

    def near_copy(offset, part):
        blocks = pl.ds(0, 1) if part == 0 else pl.ds(1, 2)
        back = tuple(-step for step in offset)
        start, rows = source_rows[offset[0]]
        goal = target_rows[back[0]][0]
        return pltpu.make_async_remote_copy(
            src_ref=packed.at[offset[2] + 1, blocks, pl.ds(start, rows), :],
            dst_ref=halo.at[back[1] + 1, back[2] + 1, blocks, pl.ds(goal, rows), :],
            send_sem=near_send.at[number(offset), part],
            recv_sem=near_recv.at[number(back), part],
            device_id=device(offset), device_id_type=MESH,
        )

    def near_arrival(offset, part):
        blocks = pl.ds(0, 1) if part == 0 else pl.ds(1, 2)
        goal, rows = target_rows[offset[0]]
        where = halo.at[offset[1] + 1, offset[2] + 1, blocks, pl.ds(goal, rows), :]
        return pltpu.make_async_remote_copy(
            src_ref=where, dst_ref=where,
            send_sem=near_send.at[number(offset), part],
            recv_sem=near_recv.at[number(offset), part],
            device_id=device(offset), device_id_type=MESH,
        )

    for load in loads[:2]:
        load.wait()

    def pack(lines_of):
        total = None
        for q, line in enumerate(lines_of):
            spread = lax.dot_general(
                line, place_ref[...], (((0,), (0,)), ((), ())),
                precision=HIGHEST, preferred_element_type=jnp.float32,
            )
            spread = [spread[:, 128 * v : 128 * (v + 1)] for v in range(3)]
            if q:
                spread = [pltpu.roll(s, SLOT * q, 1) for s in spread]
            total = spread if total is None else [t + s for t, s in zip(total, spread)]
        return total

    pairs = [(k, y) for k in range(3) for y in range(2)]
    for block, members in ((1, pairs[:4]), (2, pairs[4:])):
        spread = pack([disp_ref[k, y] for k, y in members])
        for v in range(3):
            packed[v, block] = spread[v]
        halo[1, 1, block, pl.ds(8, cells_x), :] = spread[1]
    for offset in offsets:

        @pl.when(inside(offset))
        def _():
            near_copy(offset, 1).start()

    def x_copy(step):
        return pltpu.make_async_remote_copy(
            src_ref=ref_ref.at[pl.ds(sizex - 1 if step > 0 else 0, 1)],
            dst_ref=xhalo.at[pl.ds(0 if step > 0 else 1, 1)],
            send_sem=x_send.at[0 if step > 0 else 1], recv_sem=x_recv.at[0 if step > 0 else 1],
            device_id=device((step, 0, 0)), device_id_type=MESH,
        )

    for load in loads[2:4]:
        load.wait()
    for step in (-1, 1):

        @pl.when(inside((step, 0, 0)))
        def _():
            x_copy(step).start()

    for copy in z_copies:
        copy.start()

    def bin_cell(cell, carry):
        rows = pl.multiple_of(cell * 8, 8)
        total = [None, None]
        for i in range(BIN):
            x = cell * BIN + i
            slabs = (ref_ref[x].astype(jnp.float32), def_ref[x].astype(jnp.float32))
            yrows[0, pl.ds(x, 1), :] = slabs[0][:1]
            yrows[1, pl.ds(x, 1), :] = slabs[0][sizey - 1 :]
            total = [s if t is None else t + s for t, s in zip(total, slabs)]
        for image in range(2):
            for y in range(2):
                binned[2 * image + y, pl.ds(rows, 8), :] = total[image][8 * y : 8 * y + 8]
        return carry

    lax.fori_loop(0, cells_x, bin_cell, 0)
    for load in loads[4:]:
        load.wait()
    spread = None
    for q in range(4):
        line = binned[q, pl.ds(0, cells_x, stride=8), :]
        for s in range(1, 8):
            line = line + binned[q, pl.ds(s, cells_x, stride=8), :]
        part = jnp.dot(line, bin_ref[...], precision=HIGHEST, preferred_element_type=jnp.float32)
        part = [part[:, 128 * v : 128 * (v + 1)] for v in range(3)]
        if q:
            part = [pltpu.roll(p, SLOT * q, 1) for p in part]
        spread = part if spread is None else [a + b for a, b in zip(spread, part)]
    for v in range(3):
        packed[v, 0] = spread[v]
    halo[1, 1, 0, pl.ds(8, cells_x), :] = spread[1]
    for offset in offsets:

        @pl.when(inside(offset))
        def _():
            near_copy(offset, 0).start()

    def y_copy(step):
        side = 1 if step > 0 else 0
        return pltpu.make_async_remote_copy(
            src_ref=ysend.at[side], dst_ref=yhalo.at[1 - side],
            send_sem=y_send.at[side], recv_sem=y_recv.at[1 - side],
            device_id=device((0, step, 0)), device_id_type=MESH,
        )

    ysend[...] = yrows[...].astype(jnp.bfloat16)
    for step in (-1, 1):

        @pl.when(inside((0, step, 0)))
        def _():
            y_copy(step).start()

    for part in (1, 0):
        for offset in offsets:

            @pl.when(inside(offset))
            def _():
                near_arrival(offset, part).wait_recv()

    summed = [[halo[y, 0, b] + halo[y, 1, b] + halo[y, 2, b] for b in range(3)] for y in range(3)]
    rows = cells_x + 16
    lane = lax.broadcasted_iota(jnp.int32, (rows, 128), 1)
    slot = lane // SLOT

    def centred(b, upper):
        one, two = (SLOT, 128 - SLOT) if upper else (128 - SLOT, SLOT)
        ends = jnp.where(slot == 0, pltpu.roll(summed[0][b], one, 1), pltpu.roll(summed[2][b], one, 1))
        return jnp.where(jnp.logical_or(slot == 0, slot == 3), ends, pltpu.roll(summed[1][b], two, 1))

    coarse = centred(0, False)
    deformed = centred(0, True)
    displacement = [centred(1, False), centred(1, True), centred(2, False)]
    before = jnp.where(slot < 2, summed[0][0], pltpu.roll(summed[1][0], 64, 1))
    after = jnp.where(slot < 2, summed[1][0], pltpu.roll(summed[2][0], 64, 1))
    slopes = [
        (pltpu.roll(coarse, rows - 1, 0) - pltpu.roll(coarse, 1, 0)) * 0.5,
        (after - before) * 0.5,
        (pltpu.roll(coarse, 127, 1) - pltpu.roll(coarse, 1, 1)) * 0.5,
    ]
    mismatch = deformed - coarse - (
        slopes[0] * displacement[0] + slopes[1] * displacement[1] + slopes[2] * displacement[2]
    )
    place = lane - slot * SLOT
    low = jnp.where(me[2] > 0, 1, 2)
    high = jnp.where(me[2] < nz - 1, cells_z + 2, cells_z + 1)
    keep = jnp.logical_and(place >= low, place <= high)
    keep = jnp.logical_and(keep, slot >= jnp.where(me[1] > 0, 0, 1))
    keep = jnp.logical_and(keep, slot <= jnp.where(me[1] < ny - 1, 3, 2))
    rhs = [jnp.where(keep, s * mismatch, 0.0)[8 : 8 + cells_x] for s in slopes]

    mine[...] = jnp.dot(
        sums_ref[...], jnp.concatenate(rhs, axis=0), precision=HIGHEST, preferred_element_type=jnp.float32
    )

    def peer_copy(j):
        return pltpu.make_async_remote_copy(
            src_ref=mine, dst_ref=theirs.at[me[0]],
            send_sem=peer_send.at[j], recv_sem=peer_recv.at[j],
            device_id=peer(j), device_id_type=MESH,
        )

    for j in range(1, nx):
        peer_copy(j).start()

    for step in (-1, 1):

        @pl.when(inside((step, 0, 0)))
        def _():
            x_copy(-step).wait_recv()

        @pl.when(inside((0, step, 0)))
        def _():
            y_copy(-step).wait_recv()

    framed[0] = xhalo[0]
    framed[sizex + 1] = xhalo[1]
    yout[...] = yhalo[...]

    for j in range(1, nx):
        came = pltpu.make_async_remote_copy(
            src_ref=mine, dst_ref=theirs.at[lax.rem(me[0] + nx - j, nx)],
            send_sem=peer_send.at[j], recv_sem=peer_recv.at[j],
            device_id=peer(j), device_id_type=MESH,
        )
        came.wait_recv()

    lane_of = lax.broadcasted_iota(jnp.int32, (cells_z, 128), 1)
    z_of = lax.broadcasted_iota(jnp.int32, (cells_z, 128), 0)
    sums = theirs[...].reshape(8 * nx, 128)
    for k in range(3):
        step = jnp.dot(
            table_ref[k], jnp.concatenate([rhs[k], sums], axis=0),
            precision=HIGHEST, preferred_element_type=jnp.float32,
        )
        new = displacement[k] + step
        for y in range(2):
            new_ref[k, y] = lax.dot_general(
                jnp.where(lane_of == z_of + (SLOT * (y + 1) + 2), 1.0, 0.0), new[8 : 8 + cells_x],
                (((1,), (1,)), ((), ())), precision=HIGHEST, preferred_element_type=jnp.float32,
            )
        along = jnp.dot(new, prolong_ref[...], precision=HIGHEST, preferred_element_type=jnp.float32) * 0.5
        for s in range(4):
            lines[k, s] = along[:, sizez * s : sizez * (s + 1)]

    for copy in z_copies:
        copy.wait_recv()

    for copy in z_copies:
        copy.wait_send()
    for j in range(1, nx):
        peer_copy(j).wait_send()
    for step in (-1, 1):

        @pl.when(inside((step, 0, 0)))
        def _():
            x_copy(step).wait_send()

        @pl.when(inside((0, step, 0)))
        def _():
            y_copy(step).wait_send()

    for offset in offsets:

        @pl.when(inside(offset))
        def _():
            for part in range(2):
                near_copy(offset, part).wait_send()


def combine(
    counts, chunks,
    new_in, lines, refs, defs, yhalo, zhalo,
    new_ref, out_hbm,
    out, out_sem,
):
    nz = counts[2]
    sizex, sizey, sizez = defs.shape
    cells_x = sizex // BIN
    sides = zhalo.shape[0]
    span = sizex // chunks
    at_z = lax.axis_index("gz")
    new_ref[...] = new_in[...]

    row = lax.broadcasted_iota(jnp.int32, (sizez, sizez), 0)
    column = lax.broadcasted_iota(jnp.int32, (sizez, sizez), 1)
    inner = jnp.where(row == column + 1, 1.0, 0.0) - jnp.where(row + 1 == column, 1.0, 0.0)
    from_low = jnp.where(
        jnp.logical_and(jnp.logical_and(row == sizez - 1, column == 0), at_z > 0), -1.0, 0.0
    )
    from_high = jnp.where(
        jnp.logical_and(jnp.logical_and(row == 0, column == sizez - 1), at_z < nz - 1), 1.0, 0.0
    )
    outer = [from_low + from_high] if sides == 1 else [from_low, from_high]
    across = jnp.concatenate([inner] + outer, axis=0).astype(jnp.bfloat16)

    rows = BIN * sizey
    row = lax.broadcasted_iota(jnp.int32, (rows, rows + 16), 0)
    column = lax.broadcasted_iota(jnp.int32, (rows, rows + 16), 1)
    y, slab = row % sizey, row // sizey
    after = jnp.where(y == sizey - 1, rows + 8 + slab, row + 1)
    before = jnp.where(y == 0, rows + slab, row - 1)
    along = (jnp.where(column == after, 1.0, 0.0) - jnp.where(column == before, 1.0, 0.0)).astype(jnp.bfloat16)

    third = lax.broadcasted_iota(jnp.int32, (8, sizez), 0).astype(jnp.float32)
    offset_y = (third + 0.5) / 8.0 - 0.5
    weight_low = jnp.maximum(-offset_y, 0.0)
    weight_high = jnp.maximum(offset_y, 0.0)
    weight_mid = 1.0 - jnp.abs(offset_y)

    def plane(at):
        planes = []
        for k in range(3):
            row_of = [lines[k, s, pl.ds(at, 1), :] for s in range(4)]
            planes.append(
                jnp.concatenate(
                    [
                        weight_low * row_of[c] + weight_mid * row_of[c + 1] + weight_high * row_of[c + 2]
                        for c in range(2)
                    ],
                    axis=0,
                )
            )
        return planes

    def residual(cell, carry):
        past, now = carry
        later = plane(cell + 9)
        start = pl.multiple_of(cell * BIN, BIN)
        own = refs[pl.ds(start + 1, BIN)].reshape(rows, sizez)
        sideways = [own] + [zhalo[i, pl.ds(start, BIN)].reshape(rows, sizez) for i in range(sides)]
        grad_z = jnp.dot(jnp.concatenate(sideways, axis=1), across, preferred_element_type=jnp.float32)
        ends = jnp.concatenate([yhalo[i, pl.ds(start, BIN), :].astype(jnp.float32) for i in range(2)], axis=0)
        grad_y = jnp.dot(
            along, jnp.concatenate([own, ends.astype(jnp.bfloat16)], axis=0), preferred_element_type=jnp.float32
        )
        slabs = [refs[start + i].astype(jnp.float32) for i in range(BIN + 2)]
        for i in range(BIN):
            t = (i + 0.5) / BIN - 0.5
            other = later if t > 0 else past
            field = [n + abs(t) * (o - n) for n, o in zip(now, other)]
            part = slice(i * sizey, (i + 1) * sizey)
            total = defs[start + i].astype(jnp.float32) - slabs[i + 1]
            total = total - (slabs[i + 2] - slabs[i]) * field[0]
            total = total - grad_y[part] * field[1] - grad_z[part] * field[2]
            out[start + i] = total.astype(jnp.bfloat16)
        return (now, later)

    def store(c):
        slabs = pl.ds(c * span, span)
        return pltpu.make_async_copy(out.at[slabs], out_hbm.at[slabs], out_sem.at[c])

    state = (plane(7), plane(8))
    for c in range(chunks):
        each = cells_x // chunks
        state = lax.fori_loop(c * each, (c + 1) * each, residual, state)
        store(c).start()
    for c in range(chunks):
        store(c).wait()


def on_device(counts, ref_image, def_image, displacement):
    nx, ny, nz = counts
    sizex, sizey, sizez = ref_image.shape
    cells_x, cells_z = sizex // BIN, sizez // BIN
    table, sums = inverse_table(nx, cells_x)
    place, binning, prolong = lane_tables(cells_z, sizez, 4)
    sides = 1 if nz == 2 else 2
    dma = pltpu.SemaphoreType.DMA
    vmem, anywhere = pl.BlockSpec(memory_space=pltpu.VMEM), pl.BlockSpec(memory_space=pl.ANY)
    shape = jax.ShapeDtypeStruct
    image = ref_image.shape
    cells = jnp.transpose(displacement, (0, 2, 3, 1))
    constants = (table, sums, place, binning, prolong)
    held = pl.pallas_call(
        functools.partial(exchange, counts),
        out_shape=(
            shape(cells.shape, jnp.float32),
            shape((3, 4, cells_x + 16, sizez), jnp.float32),
            shape((sizex + 2, sizey, sizez), jnp.bfloat16),
            shape(image, jnp.bfloat16),
            shape((2, sizex, sizez), jnp.bfloat16),
            shape((sides,) + image, jnp.bfloat16),
        ),
        in_specs=[pl.BlockSpec(memory_space=pltpu.HBM)] * 8,
        out_specs=(vmem,) * 5 + (anywhere,),
        scratch_shapes=[
            pltpu.VMEM(cells.shape, jnp.float32),
            pltpu.VMEM(table.shape[1:], jnp.float32),
            pltpu.VMEM(sums.shape[1:], jnp.float32),
            pltpu.VMEM(place.shape, jnp.float32),
            pltpu.VMEM(binning.shape, jnp.float32),
            pltpu.VMEM(prolong.shape, jnp.float32),
            pltpu.VMEM((4, cells_x * 8, sizez), jnp.float32),
            pltpu.VMEM((3, 3, cells_x, 128), jnp.float32),
            pltpu.VMEM((3, 3, 3, cells_x + 16, 128), jnp.float32),
            pltpu.VMEM((8, 128), jnp.float32),
            pltpu.VMEM((nx, 8, 128), jnp.float32),
            pltpu.VMEM((2, sizey, sizez), jnp.bfloat16),
            pltpu.VMEM((2, sizex, sizez), jnp.float32),
            pltpu.VMEM((2, sizex, sizez), jnp.bfloat16),
            pltpu.VMEM((2, sizex, sizez), jnp.bfloat16),
            dma((8,)),
            dma((27, 2)), dma((27, 2)), dma((nx,)), dma((nx,)),
            dma((2,)), dma((2,)), dma((2,)), dma((2,)), dma((sides,)), dma((sides,)),
        ],
        compiler_params=pltpu.CompilerParams(
            collective_id=0, has_side_effects=True, vmem_limit_bytes=16 << 20
        ),
    )(*[pltpu.with_memory_space_constraint(jnp.asarray(x), pltpu.HBM) for x in (ref_image, def_image, cells) + constants])
    chunks = 4
    new, residual = pl.pallas_call(
        functools.partial(combine, counts, chunks),
        out_shape=(shape(cells.shape, jnp.float32), shape(image, jnp.bfloat16)),
        in_specs=[vmem] * 6,
        out_specs=(vmem, anywhere),
        scratch_shapes=[pltpu.VMEM(image, jnp.bfloat16), dma((chunks,))],
        compiler_params=pltpu.CompilerParams(vmem_limit_bytes=16 << 20),
    )(*held)
    return jnp.transpose(new, (0, 3, 1, 2)), residual


def solution(mesh):
    counts = tuple(mesh.shape[axis] for axis in ("gx", "gy", "gz"))
    return jax.shard_map(
        functools.partial(on_device, counts),
        mesh=mesh,
        in_specs=(P("gx", "gy", "gz"), P("gx", "gy", "gz"), P(None, "gx", "gy", "gz")),
        out_specs=(P(None, "gx", "gy", "gz"), P("gx", "gy", "gz")),
        check_vma=False,
    )
```

```python
import functools

import jax
import jax.numpy as jnp
import numpy as np
from jax import lax
from jax.experimental import pallas as pl
from jax.experimental.pallas import tpu as pltpu
from jax.sharding import PartitionSpec as P

stiffness = 64.0
BIN = 8
SLOT = 32
MESH = pl.DeviceIdType.MESH
HIGHEST = lax.Precision.HIGHEST


def inverse_table(devices, cells):
    lines = devices * cells
    theta = np.arccosh((1.0 + 2.0 * stiffness) / (2.0 * stiffness))
    index = np.arange(lines)
    low = np.minimum(index[:, None], index[None, :])
    high = np.maximum(index[:, None], index[None, :])
    a, b, c = (low + 1) * theta, (lines - high) * theta, (lines + 1) * theta
    inverse = (
        np.exp(a + b - c) * (1 - np.exp(-2 * a)) * (1 - np.exp(-2 * b)) / (1 - np.exp(-2 * c))
        / (2.0 * stiffness * np.sinh(theta))
    )
    table = np.zeros((devices, 3, cells + 16, cells + 8 * devices))
    sums = np.zeros((devices, 8, 3 * cells))
    for me in range(devices):
        first, last = me * cells, (me + 1) * cells - 1
        own = index[first : last + 1]
        up = np.exp((own - last) * theta) * (1 - np.exp(-2 * (own + 1) * theta)) / (1 - np.exp(-2 * (last + 1) * theta))
        down = (
            np.exp((first - own) * theta)
            * (1 - np.exp(-2 * (lines - own) * theta))
            / (1 - np.exp(-2 * (lines - first) * theta))
        )
        for k in range(3):
            sums[me, 2 * k, k * cells : (k + 1) * cells] = up
            sums[me, 2 * k + 1, k * cells : (k + 1) * cells] = down
            for row in range(7, cells + 9):
                x = first + row - 8
                if x < 0 or x >= lines:
                    continue
                table[me, k, row, :cells] = inverse[x, first : last + 1]
                for peer in range(devices):
                    if peer < me:
                        table[me, k, row, cells + 8 * peer + 2 * k] = inverse[x, (peer + 1) * cells - 1]
                    if peer > me:
                        table[me, k, row, cells + 8 * peer + 2 * k + 1] = inverse[x, peer * cells]
    return table.astype(np.float32), sums.astype(np.float32)


def lane_tables(cells_z, size_z, slots):
    place = np.zeros((cells_z, 3 * 128), np.float32)
    for variant in range(3):
        for z in range(cells_z):
            lane = z + 2 - (variant - 1) * cells_z
            if 0 <= lane < cells_z + 4:
                place[z, variant * 128 + lane] = 1.0
    binning = np.repeat(place, BIN, axis=0) / 32.0
    prolong = np.zeros((128, slots * size_z), np.float32)
    for slot in range(slots):
        for fine in range(size_z):
            lane, offset = slot * SLOT + fine // BIN + 2, (fine % BIN + 0.5) / BIN - 0.5
            prolong[lane, slot * size_z + fine] = 1.0 - abs(offset)
            prolong[lane + (1 if offset >= 0 else -1), slot * size_z + fine] = abs(offset)
    return place, binning, prolong


def exchange(
    counts,
    ref_hbm, def_hbm, disp_hbm, table_hbm, sums_hbm, place_hbm, bin_hbm, prolong_hbm,
    new_ref, lines, framed, def_ref, yout, zhalo,
    disp_ref, table_ref, sums_ref, place_ref, bin_ref, prolong_ref,
    binned, packed, halo, mine, theirs, xhalo, yrows, ysend, yhalo,
    load_sem,
    near_send, near_recv, peer_send, peer_recv, x_send, x_recv, y_send, y_recv, z_send, z_recv,
):
    nx, ny, nz = counts
    sizex, sizey, sizez = def_ref.shape
    ref_ref = framed.at[pl.ds(1, sizex)]
    cells_x, cells_z = sizex // BIN, sizez // BIN
    me = (lax.axis_index("gx"), lax.axis_index("gy"), lax.axis_index("gz"))

    def inside(offset):
        good = None
        for at, step, count in zip(me, offset, counts):
            if step:
                test = at > 0 if step < 0 else at < count - 1
                good = test if good is None else jnp.logical_and(good, test)
        return good

    def device(offset):
        return {"gx": me[0] + offset[0], "gy": me[1] + offset[1], "gz": me[2] + offset[2]}

    def peer(j):
        return {"gx": lax.rem(me[0] + j, nx), "gy": me[1], "gz": me[2]}

    steps = (-1, 0, 1)
    offsets = [(i, j, k) for i in steps for j in steps for k in steps if (i, j, k) != (0, 0, 0)]

    loads = [
        pltpu.make_async_copy(hbm, held, load_sem.at[i])
        for i, (hbm, held) in enumerate(
            (
                (disp_hbm, disp_ref), (place_hbm, place_ref), (ref_hbm, ref_ref), (def_hbm, def_ref),
                (bin_hbm, bin_ref), (sums_hbm.at[me[0]], sums_ref),
                (table_hbm.at[me[0]], table_ref), (prolong_hbm, prolong_ref),
            )
        )
    ]
    for load in loads:
        load.start()
    halo[...] = jnp.zeros_like(halo)
    theirs[...] = jnp.zeros_like(theirs)
    xhalo[...] = jnp.zeros_like(xhalo)
    yhalo[...] = jnp.zeros_like(yhalo)

    z_steps = (1,) if nz == 2 else (1, nz - 1)

    def z_device(step):
        return {"gx": me[0], "gy": me[1], "gz": lax.rem(me[2] + step, nz)}

    barrier = pltpu.get_barrier_semaphore()
    for j in range(1, nx):
        pl.semaphore_signal(barrier, inc=1, device_id=peer(j), device_id_type=MESH)
    expect = jnp.int32(nx - 1)
    for offset in offsets:
        if offset[1:] == (0, 0):
            continue

        @pl.when(inside(offset))
        def _():
            pl.semaphore_signal(barrier, inc=1, device_id=device(offset), device_id_type=MESH)

    reach = [
        1 + (at > 0).astype(jnp.int32) + (at < count - 1).astype(jnp.int32)
        for at, count in zip(me, counts)
    ]
    expect = expect + reach[0] * (reach[1] * reach[2] - 1)
    if nz > 2:
        ends = jnp.logical_or(me[2] == 0, me[2] == nz - 1)

        @pl.when(ends)
        def _():
            other = {"gx": me[0], "gy": me[1], "gz": nz - 1 - me[2]}
            pl.semaphore_signal(barrier, inc=1, device_id=other, device_id_type=MESH)

        expect = expect + ends.astype(jnp.int32)
    z_copies = [
        pltpu.make_async_remote_copy(
            src_ref=ref_ref, dst_ref=zhalo.at[i], send_sem=z_send.at[i], recv_sem=z_recv.at[i],
            device_id=z_device(step), device_id_type=MESH,
        )
        for i, step in enumerate(z_steps)
    ]

    source_rows = {-1: (0, 8), 0: (0, cells_x), 1: (cells_x - 8, 8)}
    target_rows = {-1: (0, 8), 0: (8, cells_x), 1: (cells_x + 8, 8)}

    def number(offset):
        return (offset[0] + 1) * 9 + (offset[1] + 1) * 3 + offset[2] + 1

    def blocks_of(step, part):
        return pl.ds(0, 1) if part == 0 else {-1: pl.ds(1, 1), 0: pl.ds(1, 2), 1: pl.ds(2, 1)}[step]

    def near_copy(offset, part):
        blocks = blocks_of(offset[1], part)
        back = tuple(-step for step in offset)
        start, rows = source_rows[offset[0]]
        goal = target_rows[back[0]][0]
        return pltpu.make_async_remote_copy(
            src_ref=packed.at[offset[2] + 1, blocks, pl.ds(start, rows), :],
            dst_ref=halo.at[back[1] + 1, back[2] + 1, blocks, pl.ds(goal, rows), :],
            send_sem=near_send.at[number(offset), part],
            recv_sem=near_recv.at[number(back), part],
            device_id=device(offset), device_id_type=MESH,
        )

    def near_arrival(offset, part):
        blocks = blocks_of(-offset[1], part)
        goal, rows = target_rows[offset[0]]
        where = halo.at[offset[1] + 1, offset[2] + 1, blocks, pl.ds(goal, rows), :]
        return pltpu.make_async_remote_copy(
            src_ref=where, dst_ref=where,
            send_sem=near_send.at[number(offset), part],
            recv_sem=near_recv.at[number(offset), part],
            device_id=device(offset), device_id_type=MESH,
        )

    for load in loads[:2]:
        load.wait()

    def pack(lines_of):
        total = None
        for q, line in enumerate(lines_of):
            spread = lax.dot_general(
                line, place_ref[...], (((0,), (0,)), ((), ())),
                precision=HIGHEST, preferred_element_type=jnp.float32,
            )
            spread = [spread[:, 128 * v : 128 * (v + 1)] for v in range(3)]
            if q:
                spread = [pltpu.roll(s, SLOT * q, 1) for s in spread]
            total = spread if total is None else [t + s for t, s in zip(total, spread)]
        return total

    for block in (1, 2):
        spread = pack([disp_ref[k, block - 1] for k in range(3)])
        for v in range(3):
            packed[v, block] = spread[v]
        halo[1, 1, block, pl.ds(8, cells_x), :] = spread[1]
    pl.semaphore_wait(barrier, expect)
    for offset in offsets:

        @pl.when(inside(offset))
        def _():
            near_copy(offset, 1).start()

    def x_copy(step):
        return pltpu.make_async_remote_copy(
            src_ref=ref_ref.at[pl.ds(sizex - 1 if step > 0 else 0, 1)],
            dst_ref=xhalo.at[pl.ds(0 if step > 0 else 1, 1)],
            send_sem=x_send.at[0 if step > 0 else 1], recv_sem=x_recv.at[0 if step > 0 else 1],
            device_id=device((step, 0, 0)), device_id_type=MESH,
        )

    for load in loads[2:4]:
        load.wait()
    for step in (-1, 1):

        @pl.when(inside((step, 0, 0)))
        def _():
            x_copy(step).start()

    for copy in z_copies:
        copy.start()

    def bin_cell(cell, carry):
        rows = pl.multiple_of(cell * 8, 8)
        total = [None, None]
        for i in range(BIN):
            x = cell * BIN + i
            slabs = (ref_ref[x].astype(jnp.float32), def_ref[x].astype(jnp.float32))
            yrows[0, pl.ds(x, 1), :] = slabs[0][:1]
            yrows[1, pl.ds(x, 1), :] = slabs[0][sizey - 1 :]
            total = [s if t is None else t + s for t, s in zip(total, slabs)]
        for image in range(2):
            for y in range(2):
                binned[2 * image + y, pl.ds(rows, 8), :] = total[image][8 * y : 8 * y + 8]
        return carry

    lax.fori_loop(0, cells_x, bin_cell, 0)
    for load in loads[4:]:
        load.wait()
    spread = None
    for q in range(4):
        line = binned[q, pl.ds(0, cells_x, stride=8), :]
        for s in range(1, 8):
            line = line + binned[q, pl.ds(s, cells_x, stride=8), :]
        part = jnp.dot(line, bin_ref[...], precision=HIGHEST, preferred_element_type=jnp.float32)
        part = [part[:, 128 * v : 128 * (v + 1)] for v in range(3)]
        if q:
            part = [pltpu.roll(p, SLOT * q, 1) for p in part]
        spread = part if spread is None else [a + b for a, b in zip(spread, part)]
    for v in range(3):
        packed[v, 0] = spread[v]
    halo[1, 1, 0, pl.ds(8, cells_x), :] = spread[1]
    for offset in offsets:

        @pl.when(inside(offset))
        def _():
            near_copy(offset, 0).start()

    def y_copy(step):
        side = 1 if step > 0 else 0
        return pltpu.make_async_remote_copy(
            src_ref=ysend.at[side], dst_ref=yhalo.at[1 - side],
            send_sem=y_send.at[side], recv_sem=y_recv.at[1 - side],
            device_id=device((0, step, 0)), device_id_type=MESH,
        )

    ysend[...] = yrows[...].astype(jnp.bfloat16)
    for step in (-1, 1):

        @pl.when(inside((0, step, 0)))
        def _():
            y_copy(step).start()

    for part in (1, 0):
        for offset in offsets:

            @pl.when(inside(offset))
            def _():
                near_arrival(offset, part).wait_recv()

    summed = [[halo[y, 0, b] + halo[y, 1, b] + halo[y, 2, b] for b in range(3)] for y in range(3)]
    rows = cells_x + 16
    lane = lax.broadcasted_iota(jnp.int32, (rows, 128), 1)
    slot = lane // SLOT

    def centred(b, upper):
        one, two = (SLOT, 128 - SLOT) if upper else (128 - SLOT, SLOT)
        ends = jnp.where(slot == 0, pltpu.roll(summed[0][b], one, 1), pltpu.roll(summed[2][b], one, 1))
        return jnp.where(jnp.logical_or(slot == 0, slot == 3), ends, pltpu.roll(summed[1][b], two, 1))

    coarse = centred(0, False)
    deformed = centred(0, True)
    displacement = []
    for k in range(3):
        parts = [
            pltpu.roll(block, SLOT * ((s - k) % 4), 1) if s != k else block
            for s, block in enumerate((summed[0][2], summed[1][1], summed[1][2], summed[2][1]))
        ]
        displacement.append(
            jnp.where(slot < 2, jnp.where(slot == 0, parts[0], parts[1]), jnp.where(slot == 2, parts[2], parts[3]))
        )
    before = jnp.where(slot < 2, summed[0][0], pltpu.roll(summed[1][0], 64, 1))
    after = jnp.where(slot < 2, summed[1][0], pltpu.roll(summed[2][0], 64, 1))
    slopes = [
        (pltpu.roll(coarse, rows - 1, 0) - pltpu.roll(coarse, 1, 0)) * 0.5,
        (after - before) * 0.5,
        (pltpu.roll(coarse, 127, 1) - pltpu.roll(coarse, 1, 1)) * 0.5,
    ]
    mismatch = deformed - coarse - (
        slopes[0] * displacement[0] + slopes[1] * displacement[1] + slopes[2] * displacement[2]
    )
    place = lane - slot * SLOT
    low = jnp.where(me[2] > 0, 1, 2)
    high = jnp.where(me[2] < nz - 1, cells_z + 2, cells_z + 1)
    keep = jnp.logical_and(place >= low, place <= high)
    keep = jnp.logical_and(keep, slot >= jnp.where(me[1] > 0, 0, 1))
    keep = jnp.logical_and(keep, slot <= jnp.where(me[1] < ny - 1, 3, 2))
    rhs = [jnp.where(keep, s * mismatch, 0.0)[8 : 8 + cells_x] for s in slopes]

    mine[...] = jnp.dot(
        sums_ref[...], jnp.concatenate(rhs, axis=0), precision=HIGHEST, preferred_element_type=jnp.float32
    )

    def peer_copy(j):
        return pltpu.make_async_remote_copy(
            src_ref=mine, dst_ref=theirs.at[me[0]],
            send_sem=peer_send.at[j], recv_sem=peer_recv.at[j],
            device_id=peer(j), device_id_type=MESH,
        )

    for j in range(1, nx):
        peer_copy(j).start()

    for step in (-1, 1):

        @pl.when(inside((step, 0, 0)))
        def _():
            x_copy(-step).wait_recv()

        @pl.when(inside((0, step, 0)))
        def _():
            y_copy(-step).wait_recv()

    framed[0] = xhalo[0]
    framed[sizex + 1] = xhalo[1]
    yout[...] = yhalo[...]

    for j in range(1, nx):
        came = pltpu.make_async_remote_copy(
            src_ref=mine, dst_ref=theirs.at[lax.rem(me[0] + nx - j, nx)],
            send_sem=peer_send.at[j], recv_sem=peer_recv.at[j],
            device_id=peer(j), device_id_type=MESH,
        )
        came.wait_recv()

    lane_of = lax.broadcasted_iota(jnp.int32, (cells_z, 128), 1)
    z_of = lax.broadcasted_iota(jnp.int32, (cells_z, 128), 0)
    sums = theirs[...].reshape(8 * nx, 128)
    for k in range(3):
        step = jnp.dot(
            table_ref[k], jnp.concatenate([rhs[k], sums], axis=0),
            precision=HIGHEST, preferred_element_type=jnp.float32,
        )
        new = displacement[k] + step
        for y in range(2):
            new_ref[k, y] = lax.dot_general(
                jnp.where(lane_of == z_of + (SLOT * (y + 1) + 2), 1.0, 0.0), new[8 : 8 + cells_x],
                (((1,), (1,)), ((), ())), precision=HIGHEST, preferred_element_type=jnp.float32,
            )
        along = jnp.dot(new, prolong_ref[...], precision=HIGHEST, preferred_element_type=jnp.float32) * 0.5
        for s in range(4):
            lines[k, s] = along[:, sizez * s : sizez * (s + 1)]

    for copy in z_copies:
        copy.wait_recv()

    for copy in z_copies:
        copy.wait_send()
    for j in range(1, nx):
        peer_copy(j).wait_send()
    for step in (-1, 1):

        @pl.when(inside((step, 0, 0)))
        def _():
            x_copy(step).wait_send()

        @pl.when(inside((0, step, 0)))
        def _():
            y_copy(step).wait_send()

    for offset in offsets:

        @pl.when(inside(offset))
        def _():
            for part in range(2):
                near_copy(offset, part).wait_send()


def combine(
    counts, chunks,
    new_in, lines, refs, defs, yhalo, zhalo,
    new_ref, out_hbm,
    out, out_sem,
):
    nz = counts[2]
    sizex, sizey, sizez = defs.shape
    cells_x = sizex // BIN
    sides = zhalo.shape[0]
    span = sizex // chunks
    at_z = lax.axis_index("gz")
    new_ref[...] = new_in[...]

    row = lax.broadcasted_iota(jnp.int32, (sizez, sizez), 0)
    column = lax.broadcasted_iota(jnp.int32, (sizez, sizez), 1)
    inner = jnp.where(row == column + 1, 1.0, 0.0) - jnp.where(row + 1 == column, 1.0, 0.0)
    from_low = jnp.where(
        jnp.logical_and(jnp.logical_and(row == sizez - 1, column == 0), at_z > 0), -1.0, 0.0
    )
    from_high = jnp.where(
        jnp.logical_and(jnp.logical_and(row == 0, column == sizez - 1), at_z < nz - 1), 1.0, 0.0
    )
    outer = [from_low + from_high] if sides == 1 else [from_low, from_high]
    across = jnp.concatenate([inner] + outer, axis=0).astype(jnp.bfloat16)

    rows = BIN * sizey
    row = lax.broadcasted_iota(jnp.int32, (rows, rows + 16), 0)
    column = lax.broadcasted_iota(jnp.int32, (rows, rows + 16), 1)
    y, slab = row % sizey, row // sizey
    after = jnp.where(y == sizey - 1, rows + 8 + slab, row + 1)
    before = jnp.where(y == 0, rows + slab, row - 1)
    along = (jnp.where(column == after, 1.0, 0.0) - jnp.where(column == before, 1.0, 0.0)).astype(jnp.bfloat16)

    third = lax.broadcasted_iota(jnp.int32, (8, sizez), 0).astype(jnp.float32)
    offset_y = (third + 0.5) / 8.0 - 0.5
    weight_low = jnp.maximum(-offset_y, 0.0)
    weight_high = jnp.maximum(offset_y, 0.0)
    weight_mid = 1.0 - jnp.abs(offset_y)

    def plane(at):
        planes = []
        for k in range(3):
            row_of = [lines[k, s, pl.ds(at, 1), :] for s in range(4)]
            planes.append(
                jnp.concatenate(
                    [
                        weight_low * row_of[c] + weight_mid * row_of[c + 1] + weight_high * row_of[c + 2]
                        for c in range(2)
                    ],
                    axis=0,
                )
            )
        return planes

    def residual(cell, carry):
        past, now = carry
        later = plane(cell + 9)
        start = pl.multiple_of(cell * BIN, BIN)
        own = refs[pl.ds(start + 1, BIN)].reshape(rows, sizez)
        sideways = [own] + [zhalo[i, pl.ds(start, BIN)].reshape(rows, sizez) for i in range(sides)]
        grad_z = jnp.dot(jnp.concatenate(sideways, axis=1), across, preferred_element_type=jnp.float32)
        ends = jnp.concatenate([yhalo[i, pl.ds(start, BIN), :].astype(jnp.float32) for i in range(2)], axis=0)
        grad_y = jnp.dot(
            along, jnp.concatenate([own, ends.astype(jnp.bfloat16)], axis=0), preferred_element_type=jnp.float32
        )
        slabs = [refs[start + i].astype(jnp.float32) for i in range(BIN + 2)]
        for i in range(BIN):
            t = (i + 0.5) / BIN - 0.5
            other = later if t > 0 else past
            field = [n + abs(t) * (o - n) for n, o in zip(now, other)]
            part = slice(i * sizey, (i + 1) * sizey)
            total = defs[start + i].astype(jnp.float32) - slabs[i + 1]
            total = total - (slabs[i + 2] - slabs[i]) * field[0]
            total = total - grad_y[part] * field[1] - grad_z[part] * field[2]
            out[start + i] = total.astype(jnp.bfloat16)
        return (now, later)

    def store(c):
        slabs = pl.ds(c * span, span)
        return pltpu.make_async_copy(out.at[slabs], out_hbm.at[slabs], out_sem.at[c])

    state = (plane(7), plane(8))
    for c in range(chunks):
        each = cells_x // chunks
        state = lax.fori_loop(c * each, (c + 1) * each, residual, state)
        store(c).start()
    for c in range(chunks):
        store(c).wait()


def on_device(counts, ref_image, def_image, displacement):
    nx, ny, nz = counts
    sizex, sizey, sizez = ref_image.shape
    cells_x, cells_z = sizex // BIN, sizez // BIN
    table, sums = inverse_table(nx, cells_x)
    place, binning, prolong = lane_tables(cells_z, sizez, 4)
    sides = 1 if nz == 2 else 2
    dma = pltpu.SemaphoreType.DMA
    vmem, anywhere = pl.BlockSpec(memory_space=pltpu.VMEM), pl.BlockSpec(memory_space=pl.ANY)
    shape = jax.ShapeDtypeStruct
    image = ref_image.shape
    cells = jnp.transpose(displacement, (0, 2, 3, 1))
    constants = (table, sums, place, binning, prolong)
    held = pl.pallas_call(
        functools.partial(exchange, counts),
        out_shape=(
            shape(cells.shape, jnp.float32),
            shape((3, 4, cells_x + 16, sizez), jnp.float32),
            shape((sizex + 2, sizey, sizez), jnp.bfloat16),
            shape(image, jnp.bfloat16),
            shape((2, sizex, sizez), jnp.bfloat16),
            shape((sides,) + image, jnp.bfloat16),
        ),
        in_specs=[pl.BlockSpec(memory_space=pltpu.HBM)] * 8,
        out_specs=(vmem,) * 5 + (anywhere,),
        scratch_shapes=[
            pltpu.VMEM(cells.shape, jnp.float32),
            pltpu.VMEM(table.shape[1:], jnp.float32),
            pltpu.VMEM(sums.shape[1:], jnp.float32),
            pltpu.VMEM(place.shape, jnp.float32),
            pltpu.VMEM(binning.shape, jnp.float32),
            pltpu.VMEM(prolong.shape, jnp.float32),
            pltpu.VMEM((4, cells_x * 8, sizez), jnp.float32),
            pltpu.VMEM((3, 3, cells_x, 128), jnp.float32),
            pltpu.VMEM((3, 3, 3, cells_x + 16, 128), jnp.float32),
            pltpu.VMEM((8, 128), jnp.float32),
            pltpu.VMEM((nx, 8, 128), jnp.float32),
            pltpu.VMEM((2, sizey, sizez), jnp.bfloat16),
            pltpu.VMEM((2, sizex, sizez), jnp.float32),
            pltpu.VMEM((2, sizex, sizez), jnp.bfloat16),
            pltpu.VMEM((2, sizex, sizez), jnp.bfloat16),
            dma((8,)),
            dma((27, 2)), dma((27, 2)), dma((nx,)), dma((nx,)),
            dma((2,)), dma((2,)), dma((2,)), dma((2,)), dma((sides,)), dma((sides,)),
        ],
        compiler_params=pltpu.CompilerParams(
            collective_id=0, has_side_effects=True, vmem_limit_bytes=16 << 20
        ),
    )(*[pltpu.with_memory_space_constraint(jnp.asarray(x), pltpu.HBM) for x in (ref_image, def_image, cells) + constants])
    chunks = 4
    new, residual = pl.pallas_call(
        functools.partial(combine, counts, chunks),
        out_shape=(shape(cells.shape, jnp.float32), shape(image, jnp.bfloat16)),
        in_specs=[vmem] * 6,
        out_specs=(vmem, anywhere),
        scratch_shapes=[pltpu.VMEM(image, jnp.bfloat16), dma((chunks,))],
        compiler_params=pltpu.CompilerParams(vmem_limit_bytes=16 << 20),
    )(*held)
    return jnp.transpose(new, (0, 3, 1, 2)), residual


def solution(mesh):
    counts = tuple(mesh.shape[axis] for axis in ("gx", "gy", "gz"))
    return jax.shard_map(
        functools.partial(on_device, counts),
        mesh=mesh,
        in_specs=(P("gx", "gy", "gz"), P("gx", "gy", "gz"), P(None, "gx", "gy", "gz")),
        out_specs=(P(None, "gx", "gy", "gz"), P("gx", "gy", "gz")),
        check_vma=False,
    )
```
